32 devices in a mesh: lat: 4 (over y, x), ord: 4 (over z), batch: 2 (over core).
Axes of the slice: x: 2, y: 2, z: 4, core: 2. Of those that a mesh axis runs over, the one named last changes fastest.
Arguments:
- state_field: bfloat16 [512, 720, 1440], P(('batch', 'ord'), 'lat'), parts along dimension 0, may hold values from -6 to 6
- slot_order: int32 [512], replicated, may hold values from 0 to 511, each once
- legendre: bfloat16 [512, 720, 720], P(('lat', 'ord')), may hold values from -0.21875 to 0.21875
- degree_gain: float32 [720, 256], replicated, may hold values from 0.25 to 1.75
- mixing: bfloat16 [256, 256], replicated, may hold values from -0.375 to 0.375
Outputs:
- updated: bfloat16 [512, 720, 1440], P(('batch', 'ord'), 'lat'), parts along dimension 0
The draws below stay inside these ranges and needn't reach their ends.
There are 2 independent parts, one for each index of `batch`. The reference program is written for one: setup_inputs(seed, part) draws one part's arguments, and reference() takes and returns one part's arrays. A program takes and returns all parts, laid end to end along the dimension named above; an argument that names none is the same for every part. Nothing has to cross between parts.
Inputs may be any that keep to these rules, and one draw needn't show every extreme that they name: `slot_order`: each of 0 to 511 stands once.
All inputs are finite; a program needn't handle non-finite values.
Results may differ from the reference program's by a relative error of at most 0.0054.
Values may be sent and summed in bfloat16 or wider, within the bound.
No kernel may reach another device: no remote copies, remote signals or barrier semaphores. Data moves between devices by JAX's collectives and lax.ppermute only.
A program may use at most 320 MiB of HBM per device.

```python
import math
import jax
import jax.numpy as jnp
from jax import lax

C = 256
NLAT = 720
NLON = 1440
L = 720
M = 512


def level_of(own_key, shape, pieces, low, high):
    def one(axis_at, shards_of):
        steps = jax.random.uniform(jax.random.fold_in(jax.random.fold_in(own_key, 6), axis_at), (shards_of,), jnp.float32, low / len(pieces), high / len(pieces))
        return jnp.repeat(jnp.exp(steps), shape[axis_at] // shards_of).reshape((-1,) + (1,) * (len(shape) - axis_at - 1))

    level = one(*pieces[0])
    for cut in pieces[1:]:
        level = level * one(*cut)
    return level


def normal_values(key, extent, scale, bound, split=(), kind=jnp.bfloat16):
    gain = level_of(key, extent, split, -0.22, 0.18) if split else 1.0
    drawn = jax.random.normal(key, extent, jnp.float32) * scale * gain
    return jnp.minimum(jnp.maximum(drawn, -bound), bound).astype(kind)


def setup_inputs(seed: int = 0, part: int = 0) -> dict:
    seeds = jax.random.split(jax.random.key(seed), 6)
    part_splits = jax.random.split(jax.random.fold_in(seeds[5], part), 6)
    return {
        "state_field": normal_values(part_splits[0], (C, NLAT, NLON), 1.0, 6.0, ((0, 4), (1, 4))),
        "slot_order": jax.random.permutation(seeds[1], M).astype(jnp.int32),
        "legendre": normal_values(seeds[2], (M, L, NLAT), NLAT ** -0.5, 0.21875, ((0, 16),)),
        "degree_gain": jnp.clip(jax.random.uniform(seeds[3], (L, C), jnp.float32, 0.25, 1.75), 0.25, 1.75),
        "mixing": normal_values(seeds[4], (C, C), C ** -0.5, 0.375),
    }


def tables(orders, lon_count):
    longitude = jnp.arange(lon_count, dtype=jnp.int32)
    phase = longitude[:, None] * orders[None, :].astype(jnp.int32) % lon_count
    angle = phase.astype(jnp.float32) * (2.0 * math.pi / lon_count)
    root = 1.0 / math.sqrt(lon_count)
    forward = jnp.concatenate([jnp.cos(angle) * root, -jnp.sin(angle) * root], axis=1).astype(jnp.bfloat16)
    weights = jnp.where(orders == 0, 1.0, 2.0).astype(jnp.float32) * root
    inverse = jnp.concatenate([jnp.cos(angle).T * weights[:, None], -jnp.sin(angle).T * weights[:, None]], axis=0).astype(jnp.bfloat16)
    return (forward, inverse)

def reference(state_field, slot_order, legendre, degree_gain, mixing):
    high = lax.Precision.HIGHEST
    forward, inverse = tables(slot_order, NLON)
    flat = state_field.reshape(C * NLAT, NLON).astype(jnp.float32)
    fourier = jnp.dot(flat, forward.astype(jnp.float32), precision=high, preferred_element_type=jnp.float32).astype(jnp.bfloat16)
    fourier = fourier.reshape(C, NLAT, 2, M).transpose(3, 1, 2, 0).reshape(M, NLAT, 2 * C)
    padded_gain = jnp.concatenate([degree_gain, jnp.zeros((L, C), jnp.float32)], axis=0)
    mix_wide = mixing.astype(jnp.float32)

    def per_slot(item):
        slot_table, coeffs, order = item
        table_wide = slot_table.astype(jnp.float32)
        spec = jnp.dot(table_wide, coeffs.astype(jnp.float32), precision=high, preferred_element_type=jnp.float32)
        gain_rows = lax.dynamic_slice_in_dim(padded_gain, order.astype(jnp.int32), L, 0)
        kept = jnp.arange(L, dtype=jnp.int32) < (L - order).astype(jnp.int32)
        filtered = jnp.where(kept[:, None, None], spec.reshape(L, 2, C) * gain_rows[:, None, :], jnp.float32(0.0)).astype(jnp.bfloat16)
        mixed = jnp.dot(filtered.reshape(2 * L, C).astype(jnp.float32), mix_wide, precision=high, preferred_element_type=jnp.float32)
        mixed = mixed.astype(jnp.bfloat16).reshape(L, 2 * C)
        synth = jnp.dot(table_wide.T, mixed.astype(jnp.float32), precision=high, preferred_element_type=jnp.float32)
        return synth.astype(jnp.bfloat16)
    synth = lax.map(per_slot, (legendre, fourier, slot_order))
    synth = synth.reshape(M, NLAT, 2, C).transpose(3, 1, 2, 0).reshape(C * NLAT, 2 * M)
    back = jnp.dot(synth.astype(jnp.float32), inverse.astype(jnp.float32), precision=high, preferred_element_type=jnp.float32)
    back = back.reshape(C, NLAT, NLON)
    return (state_field.astype(jnp.float32) + jax.nn.gelu(back, approximate=True)).astype(jnp.bfloat16)
```

```python
import functools
import math

import jax
import jax.numpy as jnp
from jax import lax
from jax.experimental import pallas as pl
from jax.experimental.pallas import tpu as pltpu
from jax.sharding import PartitionSpec as P

LANES = 128
VMEM = 60 * 1024 * 1024


def lane_spans(lon_count):
    return [(at, min(LANES, lon_count - at)) for at in range(0, lon_count, LANES)]


def row_tables(orders, lon_count):
    blocks = -(-lon_count // LANES)
    fine = jnp.arange(LANES, dtype=jnp.int32)
    coarse = jnp.arange(blocks, dtype=jnp.int32) * LANES
    step = jnp.concatenate([fine, coarse])
    phase = orders[:, None] * step[None, :] % lon_count
    angle = phase.astype(jnp.float32) * (2.0 * math.pi / lon_count)
    return jnp.cos(angle), jnp.sin(angle)


def table_kernel(cos_ref, sin_ref, imag_ref, weight_ref, forward_ref, inverse_ref, *, lon_count):
    fine_cos = cos_ref[:, :LANES]
    fine_sin = sin_ref[:, :LANES]
    root = 1.0 / math.sqrt(lon_count)
    imag = imag_ref[...] > 0
    weight = weight_ref[...]
    for block in range(-(-lon_count // LANES)):
        start = block * LANES
        width = min(LANES, lon_count - start)
        at = LANES + block
        c = cos_ref[:, at : at + 1]
        s = sin_ref[:, at : at + 1]
        left = jnp.where(imag, -s, c)
        right = jnp.where(imag, c, s)
        value = (left * fine_cos - right * fine_sin) * root
        forward_ref[:, start : start + width] = value[:, :width].astype(jnp.bfloat16)
        inverse_ref[:, start : start + width] = (value * weight)[:, :width].astype(jnp.bfloat16)


def build_tables(orders, imag, lon_count):
    cosine, sine = row_tables(orders, lon_count)
    rows = orders.shape[0]
    weight = jnp.where(orders == 0, 1.0, 2.0).astype(jnp.float32)[:, None]
    tile = 256 if rows % 256 == 0 else rows
    out = jax.ShapeDtypeStruct((rows, lon_count), jnp.bfloat16)
    wide = cosine.shape[1]
    return pl.pallas_call(
        functools.partial(table_kernel, lon_count=lon_count),
        grid=(rows // tile,),
        in_specs=[
            pl.BlockSpec((tile, wide), lambda i: (i, 0)),
            pl.BlockSpec((tile, wide), lambda i: (i, 0)),
            pl.BlockSpec((tile, 1), lambda i: (i, 0)),
            pl.BlockSpec((tile, 1), lambda i: (i, 0)),
        ],
        out_specs=[pl.BlockSpec((tile, lon_count), lambda i: (i, 0))] * 2,
        out_shape=[out, out],
        name="tables",
    )(cosine, sine, imag[:, None], weight)


def analysis_kernel(state_ref, table_ref, out_ref, *, group):
    rows, channels, lon_count = state_ref.shape
    targets, _, slots, _ = out_ref.shape
    half = targets * slots
    for first in range(0, rows, group):
        got = lax.dot_general(
            table_ref[...],
            state_ref[first : first + group].reshape(group * channels, lon_count),
            (((1,), (1,)), ((), ())),
            preferred_element_type=jnp.float32,
        )
        for q in range(group):
            cols = got[:, q * channels : (q + 1) * channels]
            both = jnp.concatenate([cols[:half], cols[half:]], axis=1)
            out_ref[:, first + q] = both.reshape(targets, slots, 2 * channels).astype(jnp.bfloat16)


def analyse(state, table, targets, slots, tile):
    lat_rows, channels, lon_count = state.shape
    group = math.gcd(tile, max(1, 256 // channels))
    rows = 2 * targets * slots
    return pl.pallas_call(
        functools.partial(analysis_kernel, group=group),
        grid=(lat_rows // tile,),
        in_specs=[
            pl.BlockSpec((tile, channels, lon_count), lambda i: (i, 0, 0)),
            pl.BlockSpec((rows, lon_count), lambda i: (0, 0)),
        ],
        out_specs=pl.BlockSpec((targets, tile, slots, 2 * channels), lambda i: (0, i, 0, 0)),
        out_shape=jax.ShapeDtypeStruct((targets, lat_rows, slots, 2 * channels), jnp.bfloat16),
        compiler_params=pltpu.CompilerParams(vmem_limit_bytes=VMEM),
        cost_estimate=pl.CostEstimate(
            flops=2 * rows * channels * lat_rows * lon_count,
            bytes_accessed=2 * channels * lat_rows * (lon_count + rows),
            transcendentals=0,
        ),
        name="analysis",
    )(state, table)


def legendre_kernel(order_ref, in_ref, leg_ref, gain_ref, mix_ref, out_ref, wide, xb, acc, *, part):
    _, ords, lats, rows, width = in_ref.shape
    degrees = leg_ref.shape[1]
    for o in range(ords):
        for a in range(lats):
            wide[a * rows : (a + 1) * rows, o * width : (o + 1) * width] = in_ref[0, o, a].astype(
                jnp.float32
            )
    xb[...] = wide[...].astype(jnp.bfloat16)
    order = order_ref[pl.program_id(0)]
    acc[...] = jnp.zeros_like(acc)
    for start in range(0, degrees, part):

        @pl.when(start < degrees - order)
        def _():
            leg = leg_ref[0, start : start + part, :]
            spec = jnp.dot(leg, xb[...], preferred_element_type=jnp.float32)
            at = order + start
            aligned = gain_ref[pl.ds(pl.multiple_of(at // 8 * 8, 8), part + 8), :]
            gain = pltpu.roll(aligned, part + 8 - at % 8, 0)[:part]
            row = lax.broadcasted_iota(jnp.int32, spec.shape, 0) + start
            kept = jnp.where(row < degrees - order, spec * gain, 0.0).astype(jnp.bfloat16)
            mixed = jnp.dot(kept, mix_ref[...], preferred_element_type=jnp.float32)
            acc[...] += lax.dot_general(
                leg,
                mixed.astype(jnp.bfloat16),
                (((0,), (0,)), ((), ())),
                preferred_element_type=jnp.float32,
            )

    for o in range(ords):
        for a in range(lats):
            out_ref[0, o, a] = acc[
                a * rows : (a + 1) * rows, o * width : (o + 1) * width
            ].astype(jnp.bfloat16)


def legendre_stage(coeffs, legendre, orders, gain, mix, first):
    slots, ords, lats, rows, width = coeffs.shape
    degrees, latitudes = legendre.shape[1:]
    total = ords * width
    part = degrees // 3 if degrees % 48 == 0 else degrees
    block = pl.BlockSpec((1, ords, lats, rows, width), lambda s, _: (s, 0, 0, 0, 0))
    return pl.pallas_call(
        functools.partial(legendre_kernel, part=part),
        grid_spec=pltpu.PrefetchScalarGridSpec(
            num_scalar_prefetch=1,
            grid=(slots,),
            in_specs=[
                block,
                pl.BlockSpec((1, degrees, latitudes), lambda s, _: (s + first, 0, 0)),
                pl.BlockSpec(gain.shape, lambda s, _: (0, 0)),
                pl.BlockSpec(mix.shape, lambda s, _: (0, 0)),
            ],
            out_specs=block,
            scratch_shapes=[
                pltpu.VMEM((latitudes, total), jnp.float32),
                pltpu.VMEM((latitudes, total), jnp.bfloat16),
                pltpu.VMEM((latitudes, total), jnp.float32),
            ],
        ),
        out_shape=jax.ShapeDtypeStruct(coeffs.shape, jnp.bfloat16),
        compiler_params=pltpu.CompilerParams(vmem_limit_bytes=VMEM),
        cost_estimate=pl.CostEstimate(
            flops=2 * slots * degrees * total * (2 * latitudes + total),
            bytes_accessed=2 * slots * (degrees * latitudes + 2 * latitudes * total),
            transcendentals=0,
        ),
        name="legendre",
    )(orders, coeffs, legendre, gain, mix)


def synthesis_kernel(*refs, count, group):
    chunks = refs[:count]
    table_ref, state_ref, out_ref, left = refs[count:]
    rows, channels, lon_count = state_ref.shape
    for first in range(0, rows, group):
        base = 0
        for ref in chunks:
            targets, _, slots, _ = ref.shape
            half = targets * slots
            for q in range(group):
                both = ref[:, first + q].reshape(half, 2 * channels)
                cols = slice((first + q) * channels, (first + q + 1) * channels)
                left[base : base + half, cols] = both[:, :channels]
                left[base + half : base + 2 * half, cols] = both[:, channels:]
            base += 2 * half
        x = lax.dot_general(
            left[:, first * channels : (first + group) * channels],
            table_ref[...],
            (((0,), (0,)), ((), ())),
            preferred_element_type=jnp.float32,
        )
        inner = x * (math.sqrt(2.0 / math.pi) * (1.0 + 0.044715 * (x * x)))
        y = 0.5 * x * (1.0 + jnp.tanh(inner))
        own = state_ref[first : first + group].astype(jnp.float32)
        out_ref[first : first + group] = (
            own + y.reshape(group, channels, lon_count)
        ).astype(jnp.bfloat16)


def synthesise(chunks, table, state, tile):
    lat_rows, channels, lon_count = state.shape
    group = math.gcd(tile, max(1, 256 // channels))
    block = pl.BlockSpec((tile, channels, lon_count), lambda i: (i, 0, 0))
    return pl.pallas_call(
        functools.partial(synthesis_kernel, count=len(chunks), group=group),
        grid=(lat_rows // tile,),
        in_specs=[
            pl.BlockSpec((c.shape[0], tile) + c.shape[2:], lambda i: (0, i, 0, 0)) for c in chunks
        ]
        + [pl.BlockSpec(table.shape, lambda i: (0, 0)), block],
        out_specs=block,
        out_shape=jax.ShapeDtypeStruct(state.shape, jnp.bfloat16),
        scratch_shapes=[pltpu.VMEM((table.shape[0], tile * channels), jnp.bfloat16)],
        compiler_params=pltpu.CompilerParams(vmem_limit_bytes=VMEM),
        name="synthesis",
    )(*chunks, table, state)


def shards(state_field, slot_order, legendre, degree_gain, mixing):
    channels, lat_rows, lon_count = state_field.shape
    my_slots, degrees, latitudes = legendre.shape
    width = mixing.shape[0]
    lat_count = lax.axis_size("lat")
    ord_count = lax.axis_size("ord")
    targets = lat_count * ord_count
    tile = math.gcd(lat_rows, 12)
    state = state_field.transpose(1, 0, 2)
    unit = max(8, my_slots // 4)
    sizes = [unit] * (my_slots // unit)

    by_target = slot_order.reshape(targets, my_slots)
    orders, imag = [], []
    first = 0
    for size in sizes:
        piece = by_target[:, first : first + size].reshape(-1)
        orders += [piece, piece]
        imag += [jnp.zeros_like(piece), jnp.ones_like(piece)]
        first += size
    forward, inverse = build_tables(jnp.concatenate(orders), jnp.concatenate(imag), lon_count)

    mine = lax.dynamic_index_in_dim(by_target, lax.axis_index(("lat", "ord")), 0, keepdims=False)
    gain = jnp.concatenate([degree_gain, jnp.zeros((degrees + 8, width), jnp.float32)], axis=0)
    gain = jnp.broadcast_to(
        gain.reshape(-1, ord_count, 1, channels), (gain.shape[0], ord_count, 2, channels)
    ).reshape(-1, 2 * width)
    mix = (
        mixing.reshape(ord_count, 1, channels, ord_count, 1, channels)
        * jnp.eye(2, dtype=mixing.dtype).reshape(1, 2, 1, 1, 2, 1)
    ).reshape(2 * width, 2 * width)

    returned = []
    first = 0
    row = 0
    for size in sizes:
        rows = 2 * targets * size
        sent = analyse(state, forward[row : row + rows], targets, size, tile)
        got = lax.all_to_all(sent, ("lat", "ord"), split_axis=0, concat_axis=0, tiled=True)
        got = got.reshape(lat_count, ord_count, lat_rows, size, 2 * channels)
        got = got.transpose(3, 1, 0, 2, 4)
        done = legendre_stage(got, legendre, mine[first : first + size], gain, mix, first)
        back = done.transpose(2, 1, 3, 0, 4).reshape(targets, lat_rows, size, 2 * channels)
        returned.append(
            lax.all_to_all(back, ("lat", "ord"), split_axis=0, concat_axis=0, tiled=True)
        )
        first += size
        row += rows
    return synthesise(returned, inverse, state, tile).transpose(1, 0, 2)


def solution(mesh):
    placed = (P(("batch", "ord"), "lat", None), P(), P(("lat", "ord"), None, None), P(), P())
    return jax.shard_map(
        shards,
        mesh=mesh,
        in_specs=placed,
        out_specs=P(("batch", "ord"), "lat", None),
        check_vma=False,
    )
```

```python
import functools
import math

import jax
import jax.numpy as jnp
from jax import lax
from jax.experimental import pallas as pl
from jax.experimental.pallas import tpu as pltpu
from jax.sharding import PartitionSpec as P

LANES = 128
SHARE_LATE = 14
VMEM = 60 * 1024 * 1024


def lane_spans(lon_count):
    return [(at, min(LANES, lon_count - at)) for at in range(0, lon_count, LANES)]


def row_tables(orders, lon_count):
    blocks = -(-lon_count // LANES)
    fine = jnp.arange(LANES, dtype=jnp.int32)
    coarse = jnp.arange(blocks, dtype=jnp.int32) * LANES
    step = jnp.concatenate([fine, coarse])
    phase = orders[:, None] * step[None, :] % lon_count
    angle = phase.astype(jnp.float32) * (2.0 * math.pi / lon_count)
    return jnp.cos(angle), jnp.sin(angle)


def table_kernel(cos_ref, sin_ref, forward_ref, *, lon_count):
    half = cos_ref.shape[0]
    fine_cos = cos_ref[:, :LANES]
    fine_sin = sin_ref[:, :LANES]
    root = 1.0 / math.sqrt(lon_count)
    for block, (start, width) in enumerate(lane_spans(lon_count)):
        at = LANES + block
        c = cos_ref[:, at : at + 1] * root
        s = sin_ref[:, at : at + 1] * root
        real = c * fine_cos - s * fine_sin
        imag = -(s * fine_cos + c * fine_sin)
        forward_ref[:half, start : start + width] = real[:, :width].astype(jnp.bfloat16)
        forward_ref[half:, start : start + width] = imag[:, :width].astype(jnp.bfloat16)


def build_table(orders, lon_count):
    cosine, sine = row_tables(orders, lon_count)
    return pl.pallas_call(
        functools.partial(table_kernel, lon_count=lon_count),
        out_shape=jax.ShapeDtypeStruct((2 * orders.shape[0], lon_count), jnp.bfloat16),
        name="table",
    )(cosine, sine)


def analysis_kernel(state_ref, table_ref, out_ref, *, group):
    rows, channels, lon_count = state_ref.shape
    targets, _, slots, _ = out_ref.shape
    half = targets * slots
    for first in range(0, rows, group):
        got = lax.dot_general(
            table_ref[...],
            state_ref[first : first + group].reshape(group * channels, lon_count),
            (((1,), (1,)), ((), ())),
            preferred_element_type=jnp.float32,
        )
        for q in range(group):
            cols = got[:, q * channels : (q + 1) * channels]
            both = jnp.concatenate([cols[:half], cols[half:]], axis=1)
            out_ref[:, first + q] = both.reshape(targets, slots, 2 * channels).astype(jnp.bfloat16)


def analyse(state, table, targets, slots, tile):
    lat_rows, channels, lon_count = state.shape
    group = math.gcd(tile, max(1, 256 // channels))
    rows = 2 * targets * slots
    return pl.pallas_call(
        functools.partial(analysis_kernel, group=group),
        grid=(lat_rows // tile,),
        in_specs=[
            pl.BlockSpec((tile, channels, lon_count), lambda i: (i, 0, 0)),
            pl.BlockSpec((rows, lon_count), lambda i: (0, 0)),
        ],
        out_specs=pl.BlockSpec((targets, tile, slots, 2 * channels), lambda i: (0, i, 0, 0)),
        out_shape=jax.ShapeDtypeStruct((targets, lat_rows, slots, 2 * channels), jnp.bfloat16),
        compiler_params=pltpu.CompilerParams(vmem_limit_bytes=VMEM),
        cost_estimate=pl.CostEstimate(
            flops=2 * rows * channels * lat_rows * lon_count,
            bytes_accessed=2 * channels * lat_rows * (lon_count + rows),
            transcendentals=0,
        ),
        name="analysis",
    )(state, table)


def legendre_kernel(order_ref, in_ref, leg_ref, gain_ref, mix_ref, out_ref, wide, xb, acc, *, part):
    _, ords, lats, rows, width = in_ref.shape
    degrees = leg_ref.shape[1]
    for o in range(ords):
        for a in range(lats):
            wide[a * rows : (a + 1) * rows, o * width : (o + 1) * width] = in_ref[0, o, a].astype(
                jnp.float32
            )
    xb[...] = wide[...].astype(jnp.bfloat16)
    order = order_ref[pl.program_id(0)]
    acc[...] = jnp.zeros_like(acc)
    for start in range(0, degrees, part):

        @pl.when(start < degrees - order)
        def _():
            leg = leg_ref[0, start : start + part, :]
            spec = jnp.dot(leg, xb[...], preferred_element_type=jnp.float32)
            at = order + start
            aligned = gain_ref[pl.ds(pl.multiple_of(at // 8 * 8, 8), part + 8), :]
            gain = pltpu.roll(aligned, part + 8 - at % 8, 0)[:part]
            row = lax.broadcasted_iota(jnp.int32, spec.shape, 0) + start
            kept = jnp.where(row < degrees - order, spec * gain, 0.0).astype(jnp.bfloat16)
            mixed = jnp.dot(kept, mix_ref[...], preferred_element_type=jnp.float32)
            acc[...] += lax.dot_general(
                leg,
                mixed.astype(jnp.bfloat16),
                (((0,), (0,)), ((), ())),
                preferred_element_type=jnp.float32,
            )

    for o in range(ords):
        for a in range(lats):
            out_ref[0, o, a] = acc[
                a * rows : (a + 1) * rows, o * width : (o + 1) * width
            ].astype(jnp.bfloat16)


def legendre_stage(coeffs, legendre, orders, gain, mix, first):
    slots, ords, lats, rows, width = coeffs.shape
    degrees, latitudes = legendre.shape[1:]
    total = ords * width
    part = degrees // 3 if degrees % 48 == 0 else degrees
    block = pl.BlockSpec((1, ords, lats, rows, width), lambda s, _: (s, 0, 0, 0, 0))
    return pl.pallas_call(
        functools.partial(legendre_kernel, part=part),
        grid_spec=pltpu.PrefetchScalarGridSpec(
            num_scalar_prefetch=1,
            grid=(slots,),
            in_specs=[
                block,
                pl.BlockSpec((1, degrees, latitudes), lambda s, _: (s + first, 0, 0)),
                pl.BlockSpec(gain.shape, lambda s, _: (0, 0)),
                pl.BlockSpec(mix.shape, lambda s, _: (0, 0)),
            ],
            out_specs=block,
            scratch_shapes=[
                pltpu.VMEM((latitudes, total), jnp.float32),
                pltpu.VMEM((latitudes, total), jnp.bfloat16),
                pltpu.VMEM((latitudes, total), jnp.float32),
            ],
        ),
        out_shape=jax.ShapeDtypeStruct(coeffs.shape, jnp.bfloat16),
        compiler_params=pltpu.CompilerParams(vmem_limit_bytes=VMEM),
        cost_estimate=pl.CostEstimate(
            flops=2 * slots * degrees * total * (2 * latitudes + total),
            bytes_accessed=2 * slots * (degrees * latitudes + 2 * latitudes * total),
            transcendentals=0,
        ),
        name="legendre",
    )(orders, coeffs, legendre, gain, mix)


def synthesis_kernel(*refs, count, group):
    chunks = refs[:count]
    table_ref, state_ref = refs[count : count + 2]
    out_ref, left = refs[-2:]
    rows, channels, lon_count = state_ref.shape
    for first in range(0, rows, group):
        base = 0
        for ref in chunks:
            targets, _, slots, _ = ref.shape
            half = targets * slots
            for q in range(group):
                both = ref[:, first + q].reshape(half, 2 * channels)
                cols = slice((first + q) * channels, (first + q + 1) * channels)
                left[base : base + half, cols] = both[:, :channels]
                left[base + half : base + 2 * half, cols] = both[:, channels:]
            base += 2 * half
        x = lax.dot_general(
            left[:, first * channels : (first + group) * channels],
            table_ref[...],
            (((0,), (0,)), ((), ())),
            preferred_element_type=jnp.float32,
        )
        inner = x * (math.sqrt(2.0 / math.pi) * (1.0 + 0.044715 * (x * x)))
        y = 0.5 * x * (1.0 + jnp.tanh(inner))
        own = state_ref[first : first + group].astype(jnp.float32)
        out_ref[first : first + group] = (
            own + y.reshape(group, channels, lon_count)
        ).astype(jnp.bfloat16)


def synthesise(chunks, table, state, tile, starts, first, count, filled=None):
    lat_rows, channels, lon_count = state.shape
    group = math.gcd(tile, max(1, 256 // channels))
    block = pl.BlockSpec((tile, channels, lon_count), lambda i: (i + first, 0, 0))

    def rows_of(shape, start):
        return pl.BlockSpec((shape[0], tile) + shape[2:], lambda i: (0, i + first - start, 0, 0))

    operands = [*chunks, table, state]
    specs = [rows_of(c.shape, start) for c, start in zip(chunks, starts)]
    specs += [pl.BlockSpec(table.shape, lambda i: (0, 0)), block]
    aliases = {}
    if filled is not None:
        aliases = {len(operands): 0}
        operands.append(filled)
        specs.append(pl.BlockSpec(memory_space=pl.ANY))
    lats = count * tile
    return pl.pallas_call(
        functools.partial(synthesis_kernel, count=len(chunks), group=group),
        grid=(count,),
        in_specs=specs,
        out_specs=block,
        out_shape=jax.ShapeDtypeStruct(state.shape, jnp.bfloat16),
        scratch_shapes=[pltpu.VMEM((table.shape[0], tile * channels), jnp.bfloat16)],
        input_output_aliases=aliases,
        compiler_params=pltpu.CompilerParams(vmem_limit_bytes=VMEM),
        cost_estimate=pl.CostEstimate(
            flops=2 * table.shape[0] * channels * lats * lon_count,
            bytes_accessed=2 * channels * lats * (2 * lon_count + table.shape[0]),
            transcendentals=channels * lats * lon_count,
        ),
        name="synthesis",
    )(*operands)


def shards(state_field, slot_order, legendre, degree_gain, mixing):
    channels, lat_rows, lon_count = state_field.shape
    my_slots, degrees, latitudes = legendre.shape
    width = mixing.shape[0]
    lat_count = lax.axis_size("lat")
    ord_count = lax.axis_size("ord")
    targets = lat_count * ord_count
    tile = math.gcd(lat_rows, 12)
    wide_tile = math.gcd(lat_rows, 20)
    state = state_field.transpose(1, 0, 2)
    unit = max(8, my_slots // 4)
    sizes = [size for size in (unit, my_slots - unit) if size > 0]

    by_target = slot_order.reshape(targets, my_slots)

    mine = lax.dynamic_index_in_dim(by_target, lax.axis_index(("lat", "ord")), 0, keepdims=False)
    gain = jnp.concatenate([degree_gain, jnp.zeros((degrees + 8, width), jnp.float32)], axis=0)
    gain = jnp.broadcast_to(
        gain.reshape(-1, ord_count, 1, channels), (gain.shape[0], ord_count, 2, channels)
    ).reshape(-1, 2 * width)
    mix = (
        mixing.reshape(ord_count, 1, channels, ord_count, 1, channels)
        * jnp.eye(2, dtype=mixing.dtype).reshape(1, 2, 1, 1, 2, 1)
    ).reshape(2 * width, 2 * width)

    steps = lat_rows // tile
    late = max(1, SHARE_LATE * steps // 100) if steps > 1 else 0
    early_rows = (steps - late) * tile
    exchange = functools.partial(
        lax.all_to_all, axis_name=("lat", "ord"), split_axis=0, concat_axis=0, tiled=True
    )
    tables, weights, arrived = [], [], []
    first = 0
    for size in sizes:
        orders = by_target[:, first : first + size].reshape(-1)
        tables.append(build_table(orders, lon_count))
        weights += [jnp.where(orders == 0, 1.0, 2.0)] * 2
        sent = analyse(state, tables[-1], targets, size, wide_tile)
        if arrived:
            sent, arrived[-1] = lax.optimization_barrier((sent, arrived[-1]))
        arrived.append(exchange(sent))
        first += size

    backs = []
    first = 0
    for size, got in zip(sizes, arrived):
        got = got.reshape(lat_count, ord_count, lat_rows, size, 2 * channels)
        got = got.transpose(3, 1, 0, 2, 4)
        done = legendre_stage(got, legendre, mine[first : first + size], gain, mix, first)
        backs.append(done.transpose(2, 1, 3, 0, 4).reshape(targets, lat_rows, size, 2 * channels))
        first += size
    inverse = (
        jnp.concatenate(tables, axis=0) * jnp.concatenate(weights)[:, None]
    ).astype(jnp.bfloat16)

    settled = [exchange(back) for back in backs[:-1]]
    zeros = [0] * len(settled)
    if not late:
        every = settled + [exchange(backs[-1])]
        out = synthesise(every, inverse, state, tile, zeros + [0], 0, steps)
        return out.transpose(1, 0, 2)
    early, rest = backs[-1][:, :early_rows], backs[-1][:, early_rows:]
    if settled:
        early, rest, settled[-1] = lax.optimization_barrier((early, rest, settled[-1]))
    early = exchange(early)
    early, rest = lax.optimization_barrier((early, rest))
    rest = exchange(rest)
    out = synthesise(settled + [early], inverse, state, tile, zeros + [0], 0, steps - late)
    out = synthesise(
        settled + [rest], inverse, state, tile, zeros + [steps - late], steps - late, late, out
    )
    return out.transpose(1, 0, 2)


def solution(mesh):
    placed = (P(("batch", "ord"), "lat", None), P(), P(("lat", "ord"), None, None), P(), P())
    return jax.shard_map(
        shards,
        mesh=mesh,
        in_specs=placed,
        out_specs=P(("batch", "ord"), "lat", None),
        check_vma=False,
    )
```

```python
import functools
import math

import jax
import jax.numpy as jnp
from jax import lax
from jax.experimental import pallas as pl
from jax.experimental.pallas import tpu as pltpu
from jax.sharding import PartitionSpec as P

LANES = 128
SHARE_LATE = 14
VMEM = 60 * 1024 * 1024


def lane_spans(lon_count):
    return [(at, min(LANES, lon_count - at)) for at in range(0, lon_count, LANES)]


def row_tables(orders, lon_count):
    blocks = -(-lon_count // LANES)
    fine = jnp.arange(LANES, dtype=jnp.int32)
    coarse = jnp.arange(blocks, dtype=jnp.int32) * LANES
    step = jnp.concatenate([fine, coarse])
    phase = orders[:, None] * step[None, :] % lon_count
    angle = phase.astype(jnp.float32) * (2.0 * math.pi / lon_count)
    return jnp.cos(angle), jnp.sin(angle)


def table_kernel(cos_ref, sin_ref, forward_ref, *, lon_count):
    half = cos_ref.shape[0]
    fine_cos = cos_ref[:, :LANES]
    fine_sin = sin_ref[:, :LANES]
    root = 1.0 / math.sqrt(lon_count)
    for block, (start, width) in enumerate(lane_spans(lon_count)):
        at = LANES + block
        c = cos_ref[:, at : at + 1] * root
        s = sin_ref[:, at : at + 1] * root
        real = c * fine_cos - s * fine_sin
        imag = -(s * fine_cos + c * fine_sin)
        forward_ref[:half, start : start + width] = real[:, :width].astype(jnp.bfloat16)
        forward_ref[half:, start : start + width] = imag[:, :width].astype(jnp.bfloat16)


def build_table(orders, lon_count):
    cosine, sine = row_tables(orders, lon_count)
    return pl.pallas_call(
        functools.partial(table_kernel, lon_count=lon_count),
        out_shape=jax.ShapeDtypeStruct((2 * orders.shape[0], lon_count), jnp.bfloat16),
        name="table",
    )(cosine, sine)


def analysis_kernel(state_ref, table_ref, out_ref, *, group):
    rows, channels, lon_count = state_ref.shape
    targets, _, slots, _ = out_ref.shape
    half = targets * slots
    for first in range(0, rows, group):
        got = lax.dot_general(
            table_ref[...],
            state_ref[first : first + group].reshape(group * channels, lon_count),
            (((1,), (1,)), ((), ())),
            preferred_element_type=jnp.float32,
        )
        for q in range(group):
            cols = got[:, q * channels : (q + 1) * channels]
            both = jnp.concatenate([cols[:half], cols[half:]], axis=1)
            out_ref[:, first + q] = both.reshape(targets, slots, 2 * channels).astype(jnp.bfloat16)


def analyse(state, table, targets, slots, tile):
    lat_rows, channels, lon_count = state.shape
    group = math.gcd(tile, max(1, 256 // channels))
    rows = 2 * targets * slots
    return pl.pallas_call(
        functools.partial(analysis_kernel, group=group),
        grid=(lat_rows // tile,),
        in_specs=[
            pl.BlockSpec((tile, channels, lon_count), lambda i: (i, 0, 0)),
            pl.BlockSpec((rows, lon_count), lambda i: (0, 0)),
        ],
        out_specs=pl.BlockSpec((targets, tile, slots, 2 * channels), lambda i: (0, i, 0, 0)),
        out_shape=jax.ShapeDtypeStruct((targets, lat_rows, slots, 2 * channels), jnp.bfloat16),
        compiler_params=pltpu.CompilerParams(vmem_limit_bytes=VMEM),
        cost_estimate=pl.CostEstimate(
            flops=2 * rows * channels * lat_rows * lon_count,
            bytes_accessed=2 * channels * lat_rows * (lon_count + rows),
            transcendentals=0,
        ),
        name="analysis",
    )(state, table)


def legendre_kernel(order_ref, in_ref, leg_ref, gain_ref, mix_ref, out_ref, wide, xb, acc, *, part):
    _, ords, lats, rows, width = in_ref.shape
    degrees = leg_ref.shape[1]
    for o in range(ords):
        for a in range(lats):
            wide[a * rows : (a + 1) * rows, o * width : (o + 1) * width] = in_ref[0, o, a].astype(
                jnp.float32
            )
    xb[...] = wide[...].astype(jnp.bfloat16)
    order = order_ref[pl.program_id(0)]
    acc[...] = jnp.zeros_like(acc)
    for start in range(0, degrees, part):

        @pl.when(start < degrees - order)
        def _():
            leg = leg_ref[0, start : start + part, :]
            spec = jnp.dot(leg, xb[...], preferred_element_type=jnp.float32)
            at = order + start
            aligned = gain_ref[pl.ds(pl.multiple_of(at // 8 * 8, 8), part + 8), :]
            gain = pltpu.roll(aligned, part + 8 - at % 8, 0)[:part]
            row = lax.broadcasted_iota(jnp.int32, spec.shape, 0) + start
            kept = jnp.where(row < degrees - order, spec * gain, 0.0).astype(jnp.bfloat16)
            mixed = jnp.dot(kept, mix_ref[...], preferred_element_type=jnp.float32)
            acc[...] += lax.dot_general(
                leg,
                mixed.astype(jnp.bfloat16),
                (((0,), (0,)), ((), ())),
                preferred_element_type=jnp.float32,
            )

    for o in range(ords):
        for a in range(lats):
            out_ref[0, o, a] = acc[
                a * rows : (a + 1) * rows, o * width : (o + 1) * width
            ].astype(jnp.bfloat16)


def legendre_stage(coeffs, legendre, orders, gain, mix, first):
    slots, ords, lats, rows, width = coeffs.shape
    degrees, latitudes = legendre.shape[1:]
    total = ords * width
    part = degrees // 3 if degrees % 48 == 0 else degrees
    block = pl.BlockSpec((1, ords, lats, rows, width), lambda s, _: (s, 0, 0, 0, 0))
    return pl.pallas_call(
        functools.partial(legendre_kernel, part=part),
        grid_spec=pltpu.PrefetchScalarGridSpec(
            num_scalar_prefetch=1,
            grid=(slots,),
            in_specs=[
                block,
                pl.BlockSpec((1, degrees, latitudes), lambda s, _: (s + first, 0, 0)),
                pl.BlockSpec(gain.shape, lambda s, _: (0, 0)),
                pl.BlockSpec(mix.shape, lambda s, _: (0, 0)),
            ],
            out_specs=block,
            scratch_shapes=[
                pltpu.VMEM((latitudes, total), jnp.float32),
                pltpu.VMEM((latitudes, total), jnp.bfloat16),
                pltpu.VMEM((latitudes, total), jnp.float32),
            ],
        ),
        out_shape=jax.ShapeDtypeStruct(coeffs.shape, jnp.bfloat16),
        compiler_params=pltpu.CompilerParams(vmem_limit_bytes=VMEM),
        cost_estimate=pl.CostEstimate(
            flops=2 * slots * degrees * total * (2 * latitudes + total),
            bytes_accessed=2 * slots * (degrees * latitudes + 2 * latitudes * total),
            transcendentals=0,
        ),
        name="legendre",
    )(orders, coeffs, legendre, gain, mix)


def synthesis_kernel(*refs, count, group):
    chunks = refs[:count]
    table_ref, state_ref = refs[count : count + 2]
    out_ref, left = refs[-2:]
    rows, channels, lon_count = state_ref.shape
    for first in range(0, rows, group):
        base = 0
        for ref in chunks:
            targets, _, slots, _ = ref.shape
            half = targets * slots
            for q in range(group):
                both = ref[:, first + q].reshape(half, 2 * channels)
                cols = slice((first + q) * channels, (first + q + 1) * channels)
                left[base : base + half, cols] = both[:, :channels]
                left[base + half : base + 2 * half, cols] = both[:, channels:]
            base += 2 * half
        x = lax.dot_general(
            left[:, first * channels : (first + group) * channels],
            table_ref[...],
            (((0,), (0,)), ((), ())),
            preferred_element_type=jnp.float32,
        )
        inner = x * (math.sqrt(2.0 / math.pi) * (1.0 + 0.044715 * (x * x)))
        y = 0.5 * x * (1.0 + jnp.tanh(inner))
        own = state_ref[first : first + group].astype(jnp.float32)
        out_ref[first : first + group] = (
            own + y.reshape(group, channels, lon_count)
        ).astype(jnp.bfloat16)


def synthesise(chunks, table, state, tile, starts, first, count, filled=None):
    lat_rows, channels, lon_count = state.shape
    group = math.gcd(tile, max(1, 256 // channels))
    block = pl.BlockSpec((tile, channels, lon_count), lambda i: (i + first, 0, 0))

    def rows_of(shape, start):
        return pl.BlockSpec((shape[0], tile) + shape[2:], lambda i: (0, i + first - start, 0, 0))

    operands = [*chunks, table, state]
    specs = [rows_of(c.shape, start) for c, start in zip(chunks, starts)]
    specs += [pl.BlockSpec(table.shape, lambda i: (0, 0)), block]
    aliases = {}
    if filled is not None:
        aliases = {len(operands): 0}
        operands.append(filled)
        specs.append(pl.BlockSpec(memory_space=pl.ANY))
    lats = count * tile
    return pl.pallas_call(
        functools.partial(synthesis_kernel, count=len(chunks), group=group),
        grid=(count,),
        in_specs=specs,
        out_specs=block,
        out_shape=jax.ShapeDtypeStruct(state.shape, jnp.bfloat16),
        scratch_shapes=[pltpu.VMEM((table.shape[0], tile * channels), jnp.bfloat16)],
        input_output_aliases=aliases,
        compiler_params=pltpu.CompilerParams(vmem_limit_bytes=VMEM),
        cost_estimate=pl.CostEstimate(
            flops=2 * table.shape[0] * channels * lats * lon_count,
            bytes_accessed=2 * channels * lats * (2 * lon_count + table.shape[0]),
            transcendentals=channels * lats * lon_count,
        ),
        name="synthesis",
    )(*operands)


def shards(state_field, slot_order, legendre, degree_gain, mixing):
    channels, lat_rows, lon_count = state_field.shape
    my_slots, degrees, latitudes = legendre.shape
    width = mixing.shape[0]
    lat_count = lax.axis_size("lat")
    ord_count = lax.axis_size("ord")
    targets = lat_count * ord_count
    tile = math.gcd(lat_rows, 12)
    wide_tile = math.gcd(lat_rows, 20)
    state = state_field.transpose(1, 0, 2)
    unit = max(8, my_slots // 4)
    sizes = [size for size in (unit, my_slots - unit) if size > 0]

    by_target = slot_order.reshape(targets, my_slots)

    mine = lax.dynamic_index_in_dim(by_target, lax.axis_index(("lat", "ord")), 0, keepdims=False)
    gain = jnp.concatenate([degree_gain, jnp.zeros((degrees + 8, width), jnp.float32)], axis=0)
    gain = jnp.broadcast_to(
        gain.reshape(-1, ord_count, 1, channels), (gain.shape[0], ord_count, 2, channels)
    ).reshape(-1, 2 * width)
    mix = (
        mixing.reshape(ord_count, 1, channels, ord_count, 1, channels)
        * jnp.eye(2, dtype=mixing.dtype).reshape(1, 2, 1, 1, 2, 1)
    ).reshape(2 * width, 2 * width)

    steps = lat_rows // tile
    late = max(1, SHARE_LATE * steps // 100) if steps > 1 else 0
    early_rows = (steps - late) * tile
    exchange = functools.partial(
        lax.all_to_all, axis_name=("lat", "ord"), split_axis=0, concat_axis=0, tiled=True
    )
    tables, weights, arrived = [], [], []
    first = 0
    for size in sizes:
        orders = by_target[:, first : first + size].reshape(-1)
        tables.append(build_table(orders, lon_count))
        weights += [jnp.where(orders == 0, 1.0, 2.0)] * 2
        sent = analyse(state, tables[-1], targets, size, wide_tile)
        arrived.append(sent)
        first += size

    def there_and_back(got, size, first):
        got = got.reshape(lat_count, ord_count, lat_rows, size, 2 * channels)
        got = got.transpose(3, 1, 0, 2, 4)
        done = legendre_stage(got, legendre, mine[first : first + size], gain, mix, first)
        return done.transpose(2, 1, 3, 0, 4).reshape(targets, lat_rows, size, 2 * channels)

    got = exchange(arrived[0])
    if len(sizes) == 1:
        backs = [there_and_back(got, sizes[0], 0)]
    else:
        head = wide_tile
        ahead, behind = arrived[1][:, :head], arrived[1][:, head:]
        ahead, behind, got = lax.optimization_barrier((ahead, behind, got))
        ahead = exchange(ahead)
        backs = [there_and_back(got, sizes[0], 0)]
        behind, ahead, backs[0] = lax.optimization_barrier((behind, ahead, backs[0]))
        got = jnp.concatenate([ahead, exchange(behind)], axis=1)
        backs.append(there_and_back(got, sizes[1], sizes[0]))
    inverse = (
        jnp.concatenate(tables, axis=0) * jnp.concatenate(weights)[:, None]
    ).astype(jnp.bfloat16)

    settled = [exchange(back) for back in backs[:-1]]
    zeros = [0] * len(settled)
    if not late:
        every = settled + [exchange(backs[-1])]
        out = synthesise(every, inverse, state, tile, zeros + [0], 0, steps)
        return out.transpose(1, 0, 2)
    early, rest = backs[-1][:, :early_rows], backs[-1][:, early_rows:]
    if settled:
        early, rest, settled[-1] = lax.optimization_barrier((early, rest, settled[-1]))
    early = exchange(early)
    early, rest = lax.optimization_barrier((early, rest))
    rest = exchange(rest)
    out = synthesise(settled + [early], inverse, state, tile, zeros + [0], 0, steps - late)
    out = synthesise(
        settled + [rest], inverse, state, tile, zeros + [steps - late], steps - late, late, out
    )
    return out.transpose(1, 0, 2)


def solution(mesh):
    placed = (P(("batch", "ord"), "lat", None), P(), P(("lat", "ord"), None, None), P(), P())
    return jax.shard_map(
        shards,
        mesh=mesh,
        in_specs=placed,
        out_specs=P(("batch", "ord"), "lat", None),
        check_vma=False,
    )
```
